32 devices in a mesh: row: 4 (over y, x), col: 8 (over z, core).
Axes of the slice: x: 2, y: 2, z: 4, core: 2. Of those that a mesh axis runs over, the one named last changes fastest.
Arguments:
- source_blocks: float32 [8192, 24576], P('row', 'col'), may hold values from -6 to 6
Outputs:
- target_blocks: float32 [4096, 49152], P('row', 'col')
- column_sums: float32 [49152], P('col')
- frobenius: float32 [], replicated
The draws below stay inside these ranges and needn't reach their ends.
All inputs are finite; a program needn't handle non-finite values.
Results may differ from the reference program's by a relative error of at most 0.00002.
Values sent between devices are 32-bit elements; how exact they have to be, the bound alone decides.
A program may use at most 192 MiB of HBM per device.

```python
import math
import jax
import jax.numpy as jnp
from jax import lax

N = 24576
SB = 128
RB = 2
TB = 512
M = 8192
E = 12
N_ROW = 4
N_COL = 8


def strengthened(drawn, own_key, source, target, parts, factor):
    owner, partner = [(jnp.arange(drawn.shape[dim]) // (drawn.shape[dim] // parts)).reshape([-1 if axis == dim else 1 for axis in range(drawn.ndim)]) for dim in (source, target)]
    chosen = jax.random.permutation(own_key, parts)[partner]
    strong = (owner == chosen) | (owner == (partner + parts // 2) % parts)
    return jnp.where(strong, factor * drawn, drawn)


def block_scale(key, shape, cuts, smallest, top_value):
    factor_of, own = 1.0, jax.random.fold_in(key, 6)
    for dim, blocks in cuts:
        steps = jnp.exp(jax.random.uniform(jax.random.fold_in(own, dim), (blocks,), jnp.float32, smallest / len(cuts), top_value / len(cuts)))
        factor_of = factor_of * jnp.repeat(steps, shape[dim] // blocks).reshape([-1 if axis == dim else 1 for axis in range(len(shape))])
    return factor_of


def noise_with(own_key, shape, width, bound, split, heavy, held_as=jnp.bfloat16):
    array = width * jax.random.normal(own_key, shape, jnp.float32)
    if split:
        array = array * block_scale(own_key, shape, split, -0.22, 0.18)
    return jnp.clip(strengthened(array, jax.random.fold_in(own_key, 3), *heavy), -bound, bound).astype(held_as)


def setup_inputs(seed: int = 0) -> dict:
    splits = jax.random.split(jax.random.key(seed), 2)
    return {
        "source_blocks": noise_with(splits[0], (M, N), 1.0, 6.0, ((0, 4), (1, 8)), (0, 1, 8, 2.0), jnp.float32),
    }


def reference(source_blocks):
    row_count = N_ROW
    col_count = N_COL
    cells = source_blocks.reshape(row_count, M // row_count // SB, SB, col_count, N // col_count // SB, SB)
    matrix = cells.transpose(1, 0, 2, 4, 3, 5).reshape(M, N)
    pieces = matrix.reshape(RB, 2, 4, row_count // 4, TB, E, 2, col_count // 4, TB)
    target_blocks = pieces.transpose(3, 2, 0, 4, 7, 1, 6, 5, 8).reshape(M // 2, 2 * N)
    scale = 1.0 / math.sqrt(M)
    totals = lax.optimization_barrier(jnp.sum(matrix, axis=0)) * scale
    grouped = totals.reshape(E, 2, col_count // 4, TB).transpose(2, 1, 0, 3)
    column_sums = jnp.broadcast_to(grouped[:, None], (col_count // 4, 2, 2, E, TB)).reshape(2 * N)
    frobenius = jnp.sqrt(jnp.sum(matrix * matrix) / (M * N))
    return (target_blocks, column_sums, frobenius)
```

```python
import functools
import math

import jax
import jax.numpy as jnp
from jax import lax
from jax.experimental import pallas as pl
from jax.experimental.pallas import tpu as pltpu
from jax.sharding import PartitionSpec as P

SB = 128
SUB = 8
QUEUES = ((15, 8, 11, 12, 9, 10, 13, 14), (7, 2, 3, 6), (5, 1), (4,))
FLIPS = (3, 1, 0, 0)
STARTS = ((3, 2, 1, 1), (3, 1, 1, 0))
LATE = ((8, 9, 10, 11), (3, 2), (1,))
HELD = (10, 2)


def flipped(index, bits):
    low = (index % 2 + bits % 2) % 2
    high = (index // 2 + bits // 2) % 2
    return high * 2 + low


def redistribute(groups, count, scale, x, out, cols, fro, own, ring, acc, part, slots, gsq, gslots,
                 send, recv, psend, precv, gsend, grecv, osem, rsem):
    row_groups, col_groups = groups
    deep, _, _, tiles, wide = x.shape[:5]
    me_row, me_col = lax.axis_index("row"), lax.axis_index("col")
    r, g = me_row % 4, me_row // 4
    c, h = me_col % 4, me_col // 4
    me = r * 4 + c

    core = c % 2
    peers = []
    for bits in range(1, 16):
        tr, tc = flipped(r, bits % 4), flipped(c, bits // 4)
        peers.append((bits, tr, tc, {"row": g * 4 + tr, "col": h * 4 + tc}))
    others = []
    for dg in range(row_groups):
        for dh in range(col_groups):
            if dg or dh:
                og, oh = (g + dg) % row_groups, (h + dh) % col_groups
                others.append((dg * col_groups + dh, {"row": og * 4 + r, "col": oh * 4 + c}))

    barrier = pltpu.get_barrier_semaphore()
    for _, _, _, device in peers:
        pl.semaphore_signal(barrier, inc=1, device_id=device)
    for _, device in others:
        pl.semaphore_signal(barrier, inc=1, device_id=device)
    pl.semaphore_wait(barrier, len(peers) + len(others))

    queues, extra, small, tail = [], [], [], []
    for queue, flip in zip(QUEUES, FLIPS):
        queues.append([])
        extra.append([])
        for s in range(deep + 1):
            for first in queue:
                apart = first // 4 % 2
                if s == deep and apart:
                    continue
                bits = first + ((first ^ flip) - first) * core if s < deep else first
                tr, tc = flipped(r, bits % 4), flipped(c, bits // 4)
                piece, span = min(s, deep - 1), pl.ds(0, tiles)
                if s == deep - 1 and not apart:
                    span = pl.ds(0, tiles - HELD[0])
                if s == deep:
                    span = pl.ds(tiles - HELD[0], HELD[0] - HELD[1])
                bucket = queues if s < deep else extra
                bucket[-1].append(pltpu.make_async_remote_copy(
                    src_ref=x.at[piece, tc // 2, tr, span, :, tc % 2],
                    dst_ref=out.at[piece, r, span, :, c],
                    send_sem=send.at[bits, s],
                    recv_sem=recv.at[bits, s],
                    device_id={"row": g * 4 + tr, "col": h * 4 + tc},
                ))
    copies = [copy for queue in queues for copy in queue]
    waiting = [list(queue) for queue in queues]

    def start(counts):
        for queue, count in zip(waiting, counts):
            for copy in queue[:count]:
                copy.start()
            del queue[:count]

    own_in = [pltpu.make_async_copy(x.at[s, c // 2, r, :, :, c % 2], own.at[s], osem.at[s])
              for s in range(deep)]
    own_out = [pltpu.make_async_copy(own.at[s], out.at[s, r, :, :, c], osem.at[s])
               for s in range(deep)]
    blocks = deep * 8

    def load(b):
        return pltpu.make_async_copy(x.at[b // 8, b // 4 % 2, b % 4], ring.at[b % 2], rsem.at[b % 2])

    def block(b, sq):
        load(b).wait()

        def column(e, sq):
            v = ring[b % 2, :, e]
            acc[e] += jnp.sum(v, axis=0)
            return sq + jnp.sum(v * v, axis=(0, 1))

        sq = lax.fori_loop(0, wide, column, sq)

        @pl.when(b + 2 < blocks)
        def _():
            load(b + 2).start()

        return sq

    def sums():
        load(0).start()
        load(1).start()
        for copy in own_in:
            copy.start()
        acc[...] = jnp.zeros_like(acc)
        sq = lax.fori_loop(0, blocks, block, jnp.zeros((SUB, SB), jnp.float32))
        part[...] = jnp.zeros_like(part)
        for k in range(2):
            for e in range(wide):
                part[k, e:e + 1, :] = jnp.sum(acc[e, k], axis=0, keepdims=True)
            part[k, wide:wide + 1, :] = jnp.sum(sq, axis=0, keepdims=True)
        for i in range(deep):
            own_in[i].wait()
            own_out[i].start()
        for bits, tr, tc, device in peers:
            copy = pltpu.make_async_remote_copy(
                src_ref=part.at[tc % 2], dst_ref=slots.at[me],
                send_sem=psend.at[bits], recv_sem=precv.at[bits], device_id=device,
            )
            copy.start()
            small.append(copy)
        slots[me] = part[c % 2]

    def fold():
        for copy in small:
            copy.wait()
        total = slots[0, wide:wide + 1, :]
        for i in range(1, 16):
            total += slots[i, wide:wide + 1, :]
        gsq[...] = jnp.broadcast_to(total, gsq.shape)
        for q in range(4):
            s = slots[q, :wide, :]
            for p in range(1, 4):
                s += slots[p * 4 + q, :wide, :]
            cols[pl.ds(q, wide, stride=4), :] = s * scale
        for i, device in others:
            copy = pltpu.make_async_remote_copy(
                src_ref=gsq, dst_ref=gslots.at[g * col_groups + h],
                send_sem=gsend.at[i], recv_sem=grecv.at[i], device_id=device,
            )
            copy.start()
            tail.append(copy)
        gslots[g * col_groups + h] = gsq[...]
        for copy in own_out:
            copy.wait()

    start(STARTS[0])
    sums()
    start(STARTS[1])
    fold()
    start([len(queue) for queue in waiting])

    @pl.when(core == 1)
    def _():
        for copy in extra[0]:
            copy.start()
        queues[0][-1].wait_send()
        for copy in extra[1]:
            copy.start()
        extra[0][1].wait_send()
        for copy in extra[2]:
            copy.start()

    for copy in tail:
        copy.wait()
    total = gslots[0]
    for i in range(1, row_groups * col_groups):
        total += gslots[i]
    fro[...] = jnp.sqrt(jnp.broadcast_to(jnp.sum(total[0:1, :]) / count, fro.shape))
    for copy in copies:
        if copy is not queues[0][-1]:
            copy.wait()
    queues[0][-1].wait_recv()

    @pl.when(core == 0)
    def _():
        queues[0][-1].wait_send()

    @pl.when(core == 1)
    def _():
        for queue in extra:
            for copy in queue:
                if copy is not extra[0][1]:
                    copy.wait()
        extra[0][1].wait_recv()


def settle(held, cols, fro, out, cols_out, fro_out, token, scalar, sem, tail):
    copies = [pltpu.make_async_copy(held.at[i // 4, i % 4], out.at[i // 4, i % 4], sem.at[i])
              for i in range(held.shape[0] * 4)]
    copies.append(pltpu.make_async_copy(cols, cols_out, tail.at[0]))
    for copy in copies:
        copy.start()
    scalar[0, 0] = jnp.max(fro[...])
    copies.append(pltpu.make_async_copy(scalar, fro_out, tail.at[1]))
    copies[-1].start()
    token[...] = fro[...]
    for copy in copies:
        copy.wait()


def rest(x, token, land, send, recv):
    deep, _, _, tiles = x.shape[:4]
    me_row, me_col = lax.axis_index("row"), lax.axis_index("col")
    r, g = me_row % 4, me_row // 4
    c, h = me_col % 4, me_col // 4
    core = c % 2

    barrier = pltpu.get_barrier_semaphore()
    for queue in LATE:
        for bits in queue:
            tr, tc = flipped(r, bits % 4), flipped(c, bits // 4)
            pl.semaphore_signal(barrier, inc=1, device_id={"row": g * 4 + tr, "col": h * 4 + tc})
    pl.semaphore_wait(barrier, sum(len(queue) for queue in LATE))

    for side in range(2):
        many = HELD[side]

        @pl.when(core == side)
        def _():
            copies = []
            for queue in LATE:
                copies.append([])
                for bits in queue:
                    tr, tc = flipped(r, bits % 4), flipped(c, bits // 4)
                    copies[-1].append(pltpu.make_async_remote_copy(
                        src_ref=x.at[deep - 1, tc // 2, tr, pl.ds(tiles - many, many), :, tc % 2],
                        dst_ref=land.at[r, c // 2, pl.ds(0, many)],
                        send_sem=send.at[bits],
                        recv_sem=recv.at[bits],
                        device_id={"row": g * 4 + tr, "col": h * 4 + tc},
                    ))
            for copy in copies[0] + copies[1]:
                copy.start()
            copies[0][1].wait_send()
            for copy in copies[2]:
                copy.start()
            for copy in copies[0] + copies[1] + copies[2]:
                if copy is not copies[0][1]:
                    copy.wait()
            copies[0][1].wait_recv()


def finish(land, before, out, sem):
    del before
    deep, _, tiles = out.shape[:3]
    r, c = lax.axis_index("row") % 4, lax.axis_index("col") % 4
    core = c % 2
    for side in range(2):
        many = HELD[side]

        @pl.when(core == side)
        def _():
            copies = []
            for queue in LATE:
                for bits in queue:
                    sr, sc = flipped(r, bits % 4), flipped(c, bits // 4)
                    copies.append(pltpu.make_async_copy(
                        land.at[sr, sc // 2, pl.ds(0, many)],
                        out.at[deep - 1, sr, pl.ds(tiles - many, many), :, sc],
                        sem.at[bits],
                    ))
            for copy in copies:
                copy.start()
            for copy in copies:
                copy.wait()


def per_device(source_blocks):
    local_rows, local_cols = source_blocks.shape
    row_count, col_count = lax.axis_size("row"), lax.axis_size("col")
    groups = (row_count // 4, col_count // 4)
    total_rows = local_rows * row_count
    count = total_rows * local_cols * col_count
    deep, wide, tiles = local_rows // (8 * SB), local_cols // (2 * SB), SB // SUB
    x = source_blocks.reshape(local_rows // SUB, SUB, local_cols // SB, SB).transpose(0, 2, 1, 3)
    x = x.reshape(deep, 2, 4, tiles, wide, 2, SUB, SB)
    f32 = jnp.float32
    x = pltpu.with_memory_space_constraint(x, pltpu.HBM)
    rows = -(-(wide + 1) // SUB) * SUB
    n = groups[0] * groups[1]
    dma = pltpu.SemaphoreType.DMA
    out, cols, fro = pl.pallas_call(
        functools.partial(redistribute, groups, float(count), 1.0 / math.sqrt(total_rows)),
        out_shape=(
            pltpu.VMEM((deep, 4, tiles, wide, 4, SUB, SB), f32),
            jax.ShapeDtypeStruct((wide * 4, SB), f32),
            jax.ShapeDtypeStruct((SUB, SB), f32),
        ),
        in_specs=[pl.BlockSpec(memory_space=pltpu.HBM)],
        out_specs=(
            pl.BlockSpec(memory_space=pl.ANY),
            pl.BlockSpec(memory_space=pltpu.VMEM),
            pl.BlockSpec(memory_space=pltpu.VMEM),
        ),
        scratch_shapes=[
            pltpu.VMEM((deep, tiles, wide, SUB, SB), f32),
            pltpu.VMEM((2, tiles, wide, 2, SUB, SB), f32),
            pltpu.VMEM((wide, 2, SUB, SB), f32),
            pltpu.VMEM((2, rows, SB), f32),
            pltpu.VMEM((16, rows, SB), f32),
            pltpu.VMEM((SUB, SB), f32),
            pltpu.VMEM((n, SUB, SB), f32),
            dma((16, deep + 1)), dma((16, deep + 1)), dma((16,)), dma((16,)),
            dma((n,)), dma((n,)), dma((deep,)), dma((2,)),
        ],
        compiler_params=pltpu.CompilerParams(
            collective_id=0, has_side_effects=True, vmem_limit_bytes=8 * 2**20
        ),
        name="redistribute",
    )(x)
    out, cols, fro, token = pl.pallas_call(
        settle,
        out_shape=(
            pltpu.HBM(out.shape, f32),
            pltpu.HBM(cols.shape, f32),
            jax.ShapeDtypeStruct((1, 1), f32),
            jax.ShapeDtypeStruct((SUB, SB), f32),
        ),
        in_specs=[
            pl.BlockSpec(memory_space=pl.ANY),
            pl.BlockSpec(memory_space=pltpu.VMEM),
            pl.BlockSpec(memory_space=pltpu.VMEM),
        ],
        out_specs=(
            pl.BlockSpec(memory_space=pltpu.HBM),
            pl.BlockSpec(memory_space=pltpu.HBM),
            pl.BlockSpec(memory_space=pltpu.HBM),
            pl.BlockSpec(memory_space=pltpu.VMEM),
        ),
        scratch_shapes=[pltpu.SMEM((1, 1), f32), dma((deep * 4,)), dma((2,))],
        compiler_params=pltpu.CompilerParams(vmem_limit_bytes=2**20),
        name="settle",
    )(out, cols, fro)
    land = pl.pallas_call(
        rest,
        out_shape=pltpu.VMEM((4, 2, HELD[0], wide, SUB, SB), f32),
        in_specs=[pl.BlockSpec(memory_space=pltpu.HBM), pl.BlockSpec(memory_space=pl.ANY)],
        out_specs=pl.BlockSpec(memory_space=pl.ANY),
        scratch_shapes=[dma((16,)), dma((16,))],
        compiler_params=pltpu.CompilerParams(
            collective_id=1, has_side_effects=True, vmem_limit_bytes=2**20
        ),
        name="rest",
    )(x, token)
    out = pl.pallas_call(
        finish,
        out_shape=pltpu.HBM(out.shape, f32),
        in_specs=[pl.BlockSpec(memory_space=pl.ANY), pl.BlockSpec(memory_space=pltpu.HBM)],
        out_specs=pl.BlockSpec(memory_space=pltpu.HBM),
        scratch_shapes=[dma((16,))],
        input_output_aliases={1: 0},
        compiler_params=pltpu.CompilerParams(vmem_limit_bytes=2**20),
        name="finish",
    )(land, out)
    target = out.reshape(deep * 4 * tiles, wide * 4, SUB, SB).transpose(0, 2, 1, 3)
    target = target.reshape(deep * 4 * SB, wide * 4 * SB)
    return target, cols.reshape(wide * 4 * SB), fro[0, 0]


def solution(mesh):
    return jax.shard_map(
        per_device,
        mesh=mesh,
        in_specs=(P("row", "col"),),
        out_specs=(P("row", "col"), P("col"), P()),
        check_vma=False,
    )
```

```python
import functools
import math

import jax
import jax.numpy as jnp
from jax import lax
from jax.experimental import pallas as pl
from jax.experimental.pallas import tpu as pltpu
from jax.sharding import PartitionSpec as P

SB = 128
SUB = 8
QUEUES = ((15, 8, 11, 12, 9, 10, 13, 14), (7, 2, 3, 6), (5, 1), (4,))
FLIPS = (3, 1, 0, 0)
STARTS = ((3, 2, 1, 1), (3, 1, 1, 0))
NEAR = (8, 2, 1, 4)
FIRST = (8, 2, 1)
HEAD = 4
LATE = (8, 11, 10, 9, 3, 1, 2)
HELD = (10, 2)
LEAD = 2


def flipped(index, bits):
    low = (index % 2 + bits % 2) % 2
    high = (index // 2 + bits // 2) % 2
    return high * 2 + low


def places(groups):
    me_row, me_col = lax.axis_index("row"), lax.axis_index("col")
    r, g = me_row % 4, me_row // 4
    c, h = me_col % 4, me_col // 4
    peers = {}
    for bits in range(1, 16):
        tr, tc = flipped(r, bits % 4), flipped(c, bits // 4)
        peers[bits] = (tr, tc, {"row": g * 4 + tr, "col": h * 4 + tc})
    others = []
    for dg in range(groups[0]):
        for dh in range(groups[1]):
            if dg or dh:
                og, oh = (g + dg) % groups[0], (h + dh) % groups[1]
                others.append((dg * groups[1] + dh, {"row": og * 4 + r, "col": oh * 4 + c}))
    return r, c, g * groups[1] + h, peers, others


def by_core(core, run):
    for side in range(2):
        pl.when(core == side)(functools.partial(run, side))


def paired(pieces, before=None):
    for bits in LATE[:4]:
        for copy in pieces[bits]:
            copy.start()
    waited = []
    for gate, follower in ((before, 3), (pieces[11][0], 1), (pieces[10][0], 2)):
        if gate is not None:
            gate.wait_send()
            waited.append(gate)
        for copy in pieces[follower]:
            copy.start()
    return waited


def settle_all(copies, waited):
    for copy in copies:
        if not any(copy is other for other in waited):
            copy.wait_send()
        copy.wait_recv()


def cut(bits, start, many):
    if bits in (10, 11) and many > 1:
        lead = min(LEAD, many - 1)
        return [pl.ds(start, many - lead), pl.ds(start + many - lead, lead)]
    return [pl.ds(start, many)]


def redistribute(groups, scale, x, out, cols, gsq, own, ring, acc, part, slots, head,
                 send, recv, psend, precv, steps, osem, rsem, hsem):
    deep, _, _, tiles, wide = x.shape[:5]
    r, c, _, peers, _ = places(groups)
    me = r * 4 + c
    core = c % 2

    heads = []
    for i, bits in enumerate(FIRST):
        tr, tc, _ = peers[bits]
        heads.append(pltpu.make_async_copy(
            x.at[0, tc // 2, tr, pl.ds(0, HEAD), :, tc % 2], head.at[i], hsem.at[i]))
        heads[-1].start()

    def remote(bits, s, span, at):
        tr, tc, device = peers[bits]
        return pltpu.make_async_remote_copy(
            src_ref=x.at[s, tc // 2, tr, span, :, tc % 2],
            dst_ref=out.at[s, r, span, :, c],
            send_sem=send.at[bits, at],
            recv_sem=recv.at[bits, at],
            device_id=device,
        )

    barrier = pltpu.get_barrier_semaphore()
    for bits in NEAR:
        pl.semaphore_signal(barrier, inc=1, device_id=peers[bits][2])
    pl.semaphore_wait(barrier, len(NEAR))
    firsts = []
    for i, bits in enumerate(FIRST):
        heads[i].wait()
        firsts.append(pltpu.make_async_remote_copy(
            src_ref=head.at[i],
            dst_ref=out.at[0, r, pl.ds(0, HEAD), :, c],
            send_sem=send.at[bits, deep + 2],
            recv_sem=recv.at[bits, deep + 2],
            device_id=peers[bits][2],
        ))
        firsts[-1].start()
    for k in range(3):
        for bits in NEAR:
            pl.semaphore_signal(steps.at[k], inc=1, device_id=peers[bits][2])
        pl.semaphore_wait(steps.at[k], len(NEAR))

    queues, waiting, extra = [], [], []
    for side in range(2):
        queues.append([])
        for queue, flip in zip(QUEUES, FLIPS):
            queues[side].append([])
            for s in range(deep):
                for bits in queue:
                    bits ^= flip * side
                    low = HEAD if s == 0 and bits in FIRST else 0
                    high = tiles - HELD[0] if s == deep - 1 and bits // 4 % 2 == 0 else tiles
                    queues[side][-1].append(remote(bits, s, pl.ds(low, high - low), s))
        waiting.append([list(queue) for queue in queues[side]])
    for bits in LATE:
        spans = cut(bits, tiles - HELD[0], HELD[0] - HELD[1])
        extra.append((bits, [remote(bits, deep - 1, span, deep + i) for i, span in enumerate(spans)]))
    extra = dict(extra)

    def start(counts, side):
        for queue, count in zip(waiting[side], counts):
            for copy in queue[:count]:
                copy.start()
            del queue[:count]

    own_in = [pltpu.make_async_copy(x.at[s, c // 2, r, :, :, c % 2], own.at[s], osem.at[s])
              for s in range(deep)]
    own_out = [pltpu.make_async_copy(own.at[s], out.at[s, r, :, :, c], osem.at[s])
               for s in range(deep)]
    blocks = deep * 8

    def load(b):
        return pltpu.make_async_copy(x.at[b // 8, b // 4 % 2, b % 4], ring.at[b % 2], rsem.at[b % 2])

    def block(b, sq):
        load(b).wait()

        def column(e, sq):
            v = ring[b % 2, :, e]
            acc[e] += jnp.sum(v, axis=0)
            return sq + jnp.sum(v * v, axis=(0, 1))

        sq = lax.fori_loop(0, wide, column, sq)

        @pl.when(b + 2 < blocks)
        def _():
            load(b + 2).start()

        return sq

    by_core(core, functools.partial(start, STARTS[0]))
    load(0).start()
    load(1).start()
    for copy in own_in:
        copy.start()
    acc[...] = jnp.zeros_like(acc)
    sq = lax.fori_loop(0, blocks, block, jnp.zeros((SUB, SB), jnp.float32))
    part[...] = jnp.zeros_like(part)
    for k in range(2):
        for e in range(wide):
            part[k, e:e + 1, :] = jnp.sum(acc[e, k], axis=0, keepdims=True)
        part[k, wide:wide + 1, :] = jnp.sum(sq, axis=0, keepdims=True)
    for i in range(deep):
        own_in[i].wait()
        own_out[i].start()
    small = []
    for bits, (tr, tc, device) in peers.items():
        small.append(pltpu.make_async_remote_copy(
            src_ref=part.at[tc % 2], dst_ref=slots.at[me],
            send_sem=psend.at[bits], recv_sem=precv.at[bits], device_id=device,
        ))
        small[-1].start()
    slots[me] = part[c % 2]
    by_core(core, functools.partial(start, STARTS[1]))

    for copy in small:
        copy.wait()
    total = slots[0, wide:wide + 1, :]
    for i in range(1, 16):
        total += slots[i, wide:wide + 1, :]
    gsq[...] = jnp.broadcast_to(total, gsq.shape)
    for q in range(4):
        s = slots[q, :wide, :]
        for p in range(1, 4):
            s += slots[p * 4 + q, :wide, :]
        cols[pl.ds(q, wide, stride=4), :] = s * scale
    for copy in own_out:
        copy.wait()

    def finish(side):
        start([len(queue) for queue in waiting[side]], side)
        copies = firsts + [copy for queue in queues[side] for copy in queue]
        waited = []
        if side == 1:
            waited = paired(extra, queues[side][0][-1])
            copies += [copy for pieces in extra.values() for copy in pieces]
        settle_all(copies, waited)

    by_core(core, finish)


def settle(held, cols, gsq, out, cols_out, token, sem, tail):
    copies = [pltpu.make_async_copy(held.at[i // 4, i % 4], out.at[i // 4, i % 4], sem.at[i])
              for i in range(held.shape[0] * 4)]
    copies.append(pltpu.make_async_copy(cols, cols_out, tail))
    for copy in copies:
        copy.start()
    token[...] = gsq[...]
    for copy in copies:
        copy.wait()


def rest(groups, count, x, gsq, land, fro, gslots, send, recv, gsend, grecv):
    deep, _, _, tiles = x.shape[:4]
    r, c, group, peers, others = places(groups)
    core = c % 2

    barrier = pltpu.get_barrier_semaphore()
    for bits in LATE:
        pl.semaphore_signal(barrier, inc=1, device_id=peers[bits][2])
    for _, device in others:
        pl.semaphore_signal(barrier, inc=1, device_id=device)
    pl.semaphore_wait(barrier, len(LATE) + len(others))

    tail = []
    for i, device in others:
        tail.append(pltpu.make_async_remote_copy(
            src_ref=gsq, dst_ref=gslots.at[group],
            send_sem=gsend.at[i], recv_sem=grecv.at[i], device_id=device,
        ))
        tail[-1].start()
    gslots[group] = gsq[...]

    def exchange(side):
        pieces = {}
        for bits in LATE:
            tr, tc, device = peers[bits]
            pieces[bits] = []
            for i, span in enumerate(cut(bits, 0, HELD[side])):
                pieces[bits].append(pltpu.make_async_remote_copy(
                    src_ref=x.at[deep - 1, tc // 2, tr, pl.ds(tiles - HELD[side] + span.start, span.size), :, tc % 2],
                    dst_ref=land.at[r, c // 2, span],
                    send_sem=send.at[bits, i],
                    recv_sem=recv.at[bits, i],
                    device_id=device,
                ))
        waited = paired(pieces)
        settle_all([copy for copies in pieces.values() for copy in copies], waited)

    by_core(core, exchange)
    for copy in tail:
        copy.wait()
    total = gslots[0]
    for i in range(1, groups[0] * groups[1]):
        total += gslots[i]
    fro[...] = jnp.sqrt(jnp.broadcast_to(jnp.sum(total[0:1, :]) / count, fro.shape))


def finish(land, fro, before, out, fro_out, scalar, sem, tail):
    del before
    deep, _, tiles = out.shape[:3]
    r, c, _, peers, _ = places((1, 1))

    def copies(side):
        moves = []
        for bits in LATE:
            tr, tc, _ = peers[bits]
            moves.append(pltpu.make_async_copy(
                land.at[tr, tc // 2, pl.ds(0, HELD[side])],
                out.at[deep - 1, tr, pl.ds(tiles - HELD[side], HELD[side]), :, tc],
                sem.at[bits],
            ))
        return moves

    def begin(side):
        for copy in copies(side):
            copy.start()

    def end(side):
        for copy in copies(side):
            copy.wait()

    by_core(c % 2, begin)
    scalar[0, 0] = jnp.max(fro[...])
    last = pltpu.make_async_copy(scalar, fro_out, tail)
    last.start()
    by_core(c % 2, end)
    last.wait()


def per_device(source_blocks):
    local_rows, local_cols = source_blocks.shape
    row_count, col_count = lax.axis_size("row"), lax.axis_size("col")
    groups = (row_count // 4, col_count // 4)
    total_rows = local_rows * row_count
    count = total_rows * local_cols * col_count
    deep, wide, tiles = local_rows // (8 * SB), local_cols // (2 * SB), SB // SUB
    x = source_blocks.reshape(local_rows // SUB, SUB, local_cols // SB, SB).transpose(0, 2, 1, 3)
    x = x.reshape(deep, 2, 4, tiles, wide, 2, SUB, SB)
    x = pltpu.with_memory_space_constraint(x, pltpu.HBM)
    f32 = jnp.float32
    rows = -(-(wide + 1) // SUB) * SUB
    n = groups[0] * groups[1]
    dma = pltpu.SemaphoreType.DMA
    anywhere = pl.BlockSpec(memory_space=pl.ANY)
    hbm = pl.BlockSpec(memory_space=pltpu.HBM)
    vmem = pl.BlockSpec(memory_space=pltpu.VMEM)
    small = jax.ShapeDtypeStruct((SUB, SB), f32)
    held, cols, gsq = pl.pallas_call(
        functools.partial(redistribute, groups, 1.0 / math.sqrt(total_rows)),
        out_shape=(
            pltpu.VMEM((deep, 4, tiles, wide, 4, SUB, SB), f32),
            jax.ShapeDtypeStruct((wide * 4, SB), f32),
            small,
        ),
        in_specs=[hbm],
        out_specs=(anywhere, vmem, vmem),
        scratch_shapes=[
            pltpu.VMEM((deep, tiles, wide, SUB, SB), f32),
            pltpu.VMEM((2, tiles, wide, 2, SUB, SB), f32),
            pltpu.VMEM((wide, 2, SUB, SB), f32),
            pltpu.VMEM((2, rows, SB), f32),
            pltpu.VMEM((16, rows, SB), f32),
            pltpu.VMEM((len(FIRST), HEAD, wide, SUB, SB), f32),
            dma((16, deep + 3)), dma((16, deep + 3)), dma((16,)), dma((16,)),
            pltpu.SemaphoreType.REGULAR((3,)), dma((deep,)), dma((2,)), dma((len(FIRST),)),
        ],
        compiler_params=pltpu.CompilerParams(
            collective_id=0, has_side_effects=True, vmem_limit_bytes=8 * 2**20
        ),
        name="redistribute",
    )(x)
    out, cols, token = pl.pallas_call(
        settle,
        out_shape=(pltpu.HBM(held.shape, f32), pltpu.HBM(cols.shape, f32), small),
        in_specs=[anywhere, vmem, vmem],
        out_specs=(hbm, hbm, vmem),
        scratch_shapes=[dma((deep * 4,)), dma(())],
        compiler_params=pltpu.CompilerParams(vmem_limit_bytes=2**20),
        name="settle",
    )(held, cols, gsq)
    land, fro = pl.pallas_call(
        functools.partial(rest, groups, float(count)),
        out_shape=(pltpu.VMEM((4, 2, max(HELD), wide, SUB, SB), f32), small),
        in_specs=[hbm, vmem],
        out_specs=(anywhere, vmem),
        scratch_shapes=[pltpu.VMEM((n, SUB, SB), f32), dma((16, 2)), dma((16, 2)), dma((n,)), dma((n,))],
        compiler_params=pltpu.CompilerParams(
            collective_id=1, has_side_effects=True, vmem_limit_bytes=2**20
        ),
        name="rest",
    )(x, token)
    out, fro = pl.pallas_call(
        finish,
        out_shape=(pltpu.HBM(out.shape, f32), pltpu.HBM((1, 1), f32)),
        in_specs=[anywhere, vmem, hbm],
        out_specs=(hbm, hbm),
        scratch_shapes=[pltpu.SMEM((1, 1), f32), dma((16,)), dma(())],
        input_output_aliases={2: 0},
        compiler_params=pltpu.CompilerParams(vmem_limit_bytes=2**20),
        name="finish",
    )(land, fro, out)
    target = out.reshape(deep * 4 * tiles, wide * 4, SUB, SB).transpose(0, 2, 1, 3)
    target = target.reshape(deep * 4 * SB, wide * 4 * SB)
    return target, cols.reshape(wide * 4 * SB), fro[0, 0]


def solution(mesh):
    return jax.shard_map(
        per_device,
        mesh=mesh,
        in_specs=(P("row", "col"),),
        out_specs=(P("row", "col"), P("col"), P()),
        check_vma=False,
    )
```

```python
import functools
import math

import jax
import jax.numpy as jnp
from jax import lax
from jax.experimental import pallas as pl
from jax.experimental.pallas import tpu as pltpu
from jax.sharding import PartitionSpec as P

SB = 128
SUB = 8
QUEUES = ((15, 8, 11, 12, 9, 10, 13, 14), (7, 2, 3, 6), (5, 1), (4,))
FLIPS = (3, 1, 0, 0)
STARTS = ((3, 2, 1, 1), (3, 1, 1, 0))
NEAR = (8, 2, 1, 4)
FIRST = (8, 2, 1)
HEAD = 4
LATE = (8, 11, 10, 9, 3, 1, 2)
HELD = (10, 2)
LEAD = 4


def flipped(index, bits):
    low = (index % 2 + bits % 2) % 2
    high = (index // 2 + bits // 2) % 2
    return high * 2 + low


def places(groups):
    me_row, me_col = lax.axis_index("row"), lax.axis_index("col")
    r, g = me_row % 4, me_row // 4
    c, h = me_col % 4, me_col // 4
    peers = {}
    for bits in range(1, 16):
        tr, tc = flipped(r, bits % 4), flipped(c, bits // 4)
        peers[bits] = (tr, tc, {"row": g * 4 + tr, "col": h * 4 + tc})
    others = []
    for dg in range(groups[0]):
        for dh in range(groups[1]):
            if dg or dh:
                og, oh = (g + dg) % groups[0], (h + dh) % groups[1]
                others.append((dg * groups[1] + dh, {"row": og * 4 + r, "col": oh * 4 + c}))
    return r, c, g * groups[1] + h, peers, others


def by_core(core, run):
    for side in range(2):
        pl.when(core == side)(functools.partial(run, side))


def paired(pieces, before=None):
    for bits in LATE[:4]:
        for copy in pieces[bits]:
            copy.start()
    waited = []
    for gate, follower in ((before, 3), (pieces[11][0], 1), (pieces[10][0], 2)):
        if gate is not None:
            gate.wait_send()
            waited.append(gate)
        for copy in pieces[follower]:
            copy.start()
    return waited


def settle_all(copies, waited):
    for copy in copies:
        if not any(copy is other for other in waited):
            copy.wait_send()
        copy.wait_recv()


def cut(bits, start, many):
    if bits in (10, 11) and many > 1:
        lead = min(LEAD, many - 1)
        return [pl.ds(start, many - lead), pl.ds(start + many - lead, lead)]
    return [pl.ds(start, many)]


def redistribute(groups, scale, x, out, cols, gsq, own, ring, acc, part, slots, head,
                 send, recv, psend, precv, steps, osem, rsem, hsem):
    deep, _, _, tiles, wide = x.shape[:5]
    r, c, _, peers, _ = places(groups)
    me = r * 4 + c
    core = c % 2

    heads = []
    for i, bits in enumerate(FIRST):
        tr, tc, _ = peers[bits]
        heads.append(pltpu.make_async_copy(
            x.at[0, tc // 2, tr, pl.ds(0, HEAD), :, tc % 2], head.at[i], hsem.at[i]))
        heads[-1].start()

    def remote(bits, s, span, at):
        tr, tc, device = peers[bits]
        return pltpu.make_async_remote_copy(
            src_ref=x.at[s, tc // 2, tr, span, :, tc % 2],
            dst_ref=out.at[s, r, span, :, c],
            send_sem=send.at[at],
            recv_sem=recv.at[at],
            device_id=device,
        )

    barrier = pltpu.get_barrier_semaphore()
    for bits in NEAR:
        pl.semaphore_signal(barrier, inc=1, device_id=peers[bits][2])
    pl.semaphore_wait(barrier, len(NEAR))
    firsts = []
    for i, bits in enumerate(FIRST):
        heads[i].wait()
        firsts.append(pltpu.make_async_remote_copy(
            src_ref=head.at[i],
            dst_ref=out.at[0, r, pl.ds(0, HEAD), :, c],
            send_sem=send.at[15 * deep + i],
            recv_sem=recv.at[15 * deep + i],
            device_id=peers[bits][2],
        ))
        firsts[-1].start()
    for k in range(3):
        for bits in NEAR:
            pl.semaphore_signal(steps.at[k], inc=1, device_id=peers[bits][2])
        pl.semaphore_wait(steps.at[k], len(NEAR))

    queues, waiting, extra = [], [], []
    for side in range(2):
        queues.append([])
        for queue, flip in zip(QUEUES, FLIPS):
            queues[side].append([])
            for s in range(deep):
                for bits in queue:
                    bits ^= flip * side
                    low = HEAD if s == 0 and bits in FIRST else 0
                    high = tiles - HELD[0] if s == deep - 1 and bits // 4 % 2 == 0 else tiles
                    queues[side][-1].append(remote(bits, s, pl.ds(low, high - low), (bits - 1) * deep + s))
        waiting.append([list(queue) for queue in queues[side]])
    at = 15 * deep + len(FIRST)
    for bits in LATE:
        spans = cut(bits, tiles - HELD[0], HELD[0] - HELD[1])
        extra.append((bits, [remote(bits, deep - 1, span, at + i) for i, span in enumerate(spans)]))
        at += len(spans)
    extra = dict(extra)

    def start(counts, side):
        for queue, count in zip(waiting[side], counts):
            for copy in queue[:count]:
                copy.start()
            del queue[:count]

    own_in = [pltpu.make_async_copy(x.at[s, c // 2, r, :, :, c % 2], own.at[s], osem.at[s])
              for s in range(deep)]
    own_out = [pltpu.make_async_copy(own.at[s], out.at[s, r, :, :, c], osem.at[s])
               for s in range(deep)]
    blocks = deep * 8

    def load(b):
        return pltpu.make_async_copy(x.at[b // 8, b // 4 % 2, b % 4], ring.at[b % 2], rsem.at[b % 2])

    def block(b, sq):
        load(b).wait()

        def column(e, sq):
            v = ring[b % 2, :, e]
            acc[e] += jnp.sum(v, axis=0)
            return sq + jnp.sum(v * v, axis=(0, 1))

        sq = lax.fori_loop(0, wide, column, sq)

        @pl.when(b + 2 < blocks)
        def _():
            load(b + 2).start()

        return sq

    by_core(core, functools.partial(start, STARTS[0]))
    load(0).start()
    load(1).start()
    for copy in own_in:
        copy.start()
    acc[...] = jnp.zeros_like(acc)
    sq = lax.fori_loop(0, blocks, block, jnp.zeros((SUB, SB), jnp.float32))
    part[...] = jnp.zeros_like(part)
    for k in range(2):
        for e in range(wide):
            part[k, e:e + 1, :] = jnp.sum(acc[e, k], axis=0, keepdims=True)
        part[k, wide:wide + 1, :] = jnp.sum(sq, axis=0, keepdims=True)
    for i in range(deep):
        own_in[i].wait()
        own_out[i].start()
    small = []
    for bits, (tr, tc, device) in peers.items():
        small.append(pltpu.make_async_remote_copy(
            src_ref=part.at[tc % 2], dst_ref=slots.at[me],
            send_sem=psend.at[bits], recv_sem=precv.at[bits], device_id=device,
        ))
        small[-1].start()
    slots[me] = part[c % 2]
    by_core(core, functools.partial(start, STARTS[1]))

    for copy in small:
        copy.wait()
    total = slots[0, wide:wide + 1, :]
    for i in range(1, 16):
        total += slots[i, wide:wide + 1, :]
    gsq[...] = jnp.broadcast_to(total, gsq.shape)
    for q in range(4):
        s = slots[q, :wide, :]
        for p in range(1, 4):
            s += slots[p * 4 + q, :wide, :]
        cols[pl.ds(q, wide, stride=4), :] = s * scale
    for copy in own_out:
        copy.wait()

    def finish(side):
        start([len(queue) for queue in waiting[side]], side)
        copies = firsts + [copy for queue in queues[side] for copy in queue]
        waited = []
        if side == 1:
            waited = paired(extra, queues[side][0][-1])
            copies += [copy for pieces in extra.values() for copy in pieces]
        settle_all(copies, waited)

    by_core(core, finish)


def settle(held, cols, gsq, out, cols_out, token, sem, tail):
    copies = [pltpu.make_async_copy(held.at[i // 4, i % 4], out.at[i // 4, i % 4], sem.at[i])
              for i in range(held.shape[0] * 4)]
    copies.append(pltpu.make_async_copy(cols, cols_out, tail))
    for copy in copies:
        copy.start()
    token[...] = gsq[...]
    for copy in copies:
        copy.wait()


def rest(groups, count, x, gsq, land, fro, gslots, send, recv, gsend, grecv):
    deep, _, _, tiles = x.shape[:4]
    r, c, group, peers, others = places(groups)
    core = c % 2

    barrier = pltpu.get_barrier_semaphore()
    for bits in LATE:
        pl.semaphore_signal(barrier, inc=1, device_id=peers[bits][2])
    for _, device in others:
        pl.semaphore_signal(barrier, inc=1, device_id=device)
    pl.semaphore_wait(barrier, len(LATE) + len(others))

    tail = []
    for i, device in others:
        tail.append(pltpu.make_async_remote_copy(
            src_ref=gsq, dst_ref=gslots.at[group],
            send_sem=gsend.at[i], recv_sem=grecv.at[i], device_id=device,
        ))
        tail[-1].start()
    gslots[group] = gsq[...]

    def exchange(side):
        pieces, at = {}, 0
        for bits in LATE:
            tr, tc, device = peers[bits]
            pieces[bits] = []
            for i, span in enumerate(cut(bits, 0, HELD[side])):
                pieces[bits].append(pltpu.make_async_remote_copy(
                    src_ref=x.at[deep - 1, tc // 2, tr, pl.ds(tiles - HELD[side] + span.start, span.size), :, tc % 2],
                    dst_ref=land.at[r, c // 2, span],
                    send_sem=send.at[at],
                    recv_sem=recv.at[at],
                    device_id=device,
                ))
                at += 1
        waited = paired(pieces)
        settle_all([copy for copies in pieces.values() for copy in copies], waited)

    by_core(core, exchange)
    for copy in tail:
        copy.wait()
    total = gslots[0]
    for i in range(1, groups[0] * groups[1]):
        total += gslots[i]
    fro[...] = jnp.sqrt(jnp.broadcast_to(jnp.sum(total[0:1, :]) / count, fro.shape))


def finish(land, fro, before, out, fro_out, scalar, sem, tail):
    del before
    deep, _, tiles = out.shape[:3]
    r, c, _, peers, _ = places((1, 1))

    def copies(side):
        moves = []
        for i, bits in enumerate(LATE):
            tr, tc, _ = peers[bits]
            moves.append(pltpu.make_async_copy(
                land.at[tr, tc // 2, pl.ds(0, HELD[side])],
                out.at[deep - 1, tr, pl.ds(tiles - HELD[side], HELD[side]), :, tc],
                sem.at[i],
            ))
        return moves

    def begin(side):
        for copy in copies(side):
            copy.start()

    def end(side):
        for copy in copies(side):
            copy.wait()

    by_core(c % 2, begin)
    scalar[0, 0] = jnp.max(fro[...])
    last = pltpu.make_async_copy(scalar, fro_out, tail)
    last.start()
    by_core(c % 2, end)
    last.wait()


def per_device(source_blocks):
    local_rows, local_cols = source_blocks.shape
    row_count, col_count = lax.axis_size("row"), lax.axis_size("col")
    groups = (row_count // 4, col_count // 4)
    total_rows = local_rows * row_count
    count = total_rows * local_cols * col_count
    deep, wide, tiles = local_rows // (8 * SB), local_cols // (2 * SB), SB // SUB
    x = source_blocks.reshape(local_rows // SUB, SUB, local_cols // SB, SB).transpose(0, 2, 1, 3)
    x = x.reshape(deep, 2, 4, tiles, wide, 2, SUB, SB)
    x = pltpu.with_memory_space_constraint(x, pltpu.HBM)
    f32 = jnp.float32
    rows = -(-(wide + 1) // SUB) * SUB
    n = groups[0] * groups[1]
    dma = pltpu.SemaphoreType.DMA
    anywhere = pl.BlockSpec(memory_space=pl.ANY)
    hbm = pl.BlockSpec(memory_space=pltpu.HBM)
    vmem = pl.BlockSpec(memory_space=pltpu.VMEM)
    small = jax.ShapeDtypeStruct((SUB, SB), f32)
    held, cols, gsq = pl.pallas_call(
        functools.partial(redistribute, groups, 1.0 / math.sqrt(total_rows)),
        out_shape=(
            pltpu.VMEM((deep, 4, tiles, wide, 4, SUB, SB), f32),
            jax.ShapeDtypeStruct((wide * 4, SB), f32),
            small,
        ),
        in_specs=[hbm],
        out_specs=(anywhere, vmem, vmem),
        scratch_shapes=[
            pltpu.VMEM((deep, tiles, wide, SUB, SB), f32),
            pltpu.VMEM((2, tiles, wide, 2, SUB, SB), f32),
            pltpu.VMEM((wide, 2, SUB, SB), f32),
            pltpu.VMEM((2, rows, SB), f32),
            pltpu.VMEM((16, rows, SB), f32),
            pltpu.VMEM((len(FIRST), HEAD, wide, SUB, SB), f32),
            dma((15 * deep + 12,)), dma((15 * deep + 12,)), dma((16,)), dma((16,)),
            pltpu.SemaphoreType.REGULAR((3,)), dma((deep,)), dma((2,)), dma((len(FIRST),)),
        ],
        compiler_params=pltpu.CompilerParams(
            collective_id=0, has_side_effects=True, vmem_limit_bytes=8 * 2**20
        ),
        name="redistribute",
    )(x)
    out, cols, token = pl.pallas_call(
        settle,
        out_shape=(pltpu.HBM(held.shape, f32), pltpu.HBM(cols.shape, f32), small),
        in_specs=[anywhere, vmem, vmem],
        out_specs=(hbm, hbm, vmem),
        scratch_shapes=[dma((deep * 4,)), dma(())],
        compiler_params=pltpu.CompilerParams(vmem_limit_bytes=2**20),
        name="settle",
    )(held, cols, gsq)
    land, fro = pl.pallas_call(
        functools.partial(rest, groups, float(count)),
        out_shape=(pltpu.VMEM((4, 2, max(HELD), wide, SUB, SB), f32), small),
        in_specs=[hbm, vmem],
        out_specs=(anywhere, vmem),
        scratch_shapes=[pltpu.VMEM((n, SUB, SB), f32), dma((9,)), dma((9,)), dma((n,)), dma((n,))],
        compiler_params=pltpu.CompilerParams(
            collective_id=1, has_side_effects=True, vmem_limit_bytes=2**20
        ),
        name="rest",
    )(x, token)
    out, fro = pl.pallas_call(
        finish,
        out_shape=(pltpu.HBM(out.shape, f32), pltpu.HBM((1, 1), f32)),
        in_specs=[anywhere, vmem, hbm],
        out_specs=(hbm, hbm),
        scratch_shapes=[pltpu.SMEM((1, 1), f32), dma((len(LATE),)), dma(())],
        input_output_aliases={2: 0},
        compiler_params=pltpu.CompilerParams(vmem_limit_bytes=2**20),
        name="finish",
    )(land, fro, out)
    target = out.reshape(deep * 4 * tiles, wide * 4, SUB, SB).transpose(0, 2, 1, 3)
    target = target.reshape(deep * 4 * SB, wide * 4 * SB)
    return target, cols.reshape(wide * 4 * SB), fro[0, 0]


def solution(mesh):
    return jax.shard_map(
        per_device,
        mesh=mesh,
        in_specs=(P("row", "col"),),
        out_specs=(P("row", "col"), P("col"), P()),
        check_vma=False,
    )
```

```python
import functools
import math

import jax
import jax.numpy as jnp
from jax import lax
from jax.experimental import pallas as pl
from jax.experimental.pallas import tpu as pltpu
from jax.sharding import PartitionSpec as P

SB = 128
SUB = 8
QUEUES = ((15, 8, 11, 12, 9, 10, 13, 14), (7, 2, 3, 6), (5, 1), (4,))
FLIPS = (3, 1, 0, 0)
STARTS = ((3, 2, 1, 1), (3, 1, 1, 0))
NEAR = (8, 2, 1, 4)
FIRST = (8, 2, 1)
HEAD = 4
LATE = (8, 11, 10, 9, 3, 1, 2)
HELD = (9, 1)
LEAD = 4


def flipped(index, bits):
    low = (index % 2 + bits % 2) % 2
    high = (index // 2 + bits // 2) % 2
    return high * 2 + low


def places(groups):
    me_row, me_col = lax.axis_index("row"), lax.axis_index("col")
    r, g = me_row % 4, me_row // 4
    c, h = me_col % 4, me_col // 4
    peers = {}
    for bits in range(1, 16):
        tr, tc = flipped(r, bits % 4), flipped(c, bits // 4)
        peers[bits] = (tr, tc, {"row": g * 4 + tr, "col": h * 4 + tc})
    others = []
    for dg in range(groups[0]):
        for dh in range(groups[1]):
            if dg or dh:
                og, oh = (g + dg) % groups[0], (h + dh) % groups[1]
                others.append((dg * groups[1] + dh, {"row": og * 4 + r, "col": oh * 4 + c}))
    return r, c, g * groups[1] + h, peers, others


def by_core(core, run):
    for side in range(2):
        pl.when(core == side)(functools.partial(run, side))


def chained(pieces, before):
    for bits in (8, 9, 10, 11):
        for copy in pieces[bits]:
            copy.start()
    before.wait_send()
    for bits in (3, 2):
        for copy in pieces[bits]:
            copy.start()
    pieces[9][0].wait_send()
    for copy in pieces[1]:
        copy.start()
    return [before, pieces[9][0]]


def paired(pieces):
    for bits in (8, 11, 10, 9, 3):
        for copy in pieces[bits]:
            copy.start()
    waited = []
    for gate, follower in ((11, 1), (10, 2)):
        pieces[gate][0].wait_send()
        waited.append(pieces[gate][0])
        for copy in pieces[follower]:
            copy.start()
    return waited


def settle_all(copies, waited):
    for copy in copies:
        if not any(copy is other for other in waited):
            copy.wait_send()
        copy.wait_recv()


def cut(split, start, many):
    if split and many > 1:
        lead = min(LEAD, many - 1)
        return [pl.ds(start, many - lead), pl.ds(start + many - lead, lead)]
    return [pl.ds(start, many)]


def redistribute(groups, scale, x, out, cols, gsq, own, ring, acc, part, slots, head,
                 send, recv, psend, precv, steps, osem, rsem, hsem):
    deep, _, _, tiles, wide = x.shape[:5]
    r, c, _, peers, _ = places(groups)
    me = r * 4 + c
    core = c % 2

    heads = []
    for i, bits in enumerate(FIRST):
        tr, tc, _ = peers[bits]
        heads.append(pltpu.make_async_copy(
            x.at[0, tc // 2, tr, pl.ds(0, HEAD), :, tc % 2], head.at[i], hsem.at[i]))
        heads[-1].start()

    def remote(bits, s, span, at):
        tr, tc, device = peers[bits]
        return pltpu.make_async_remote_copy(
            src_ref=x.at[s, tc // 2, tr, span, :, tc % 2],
            dst_ref=out.at[s, r, span, :, c],
            send_sem=send.at[at],
            recv_sem=recv.at[at],
            device_id=device,
        )

    barrier = pltpu.get_barrier_semaphore()
    for bits in NEAR:
        pl.semaphore_signal(barrier, inc=1, device_id=peers[bits][2])
    pl.semaphore_wait(barrier, len(NEAR))
    firsts = []
    for i, bits in enumerate(FIRST):
        heads[i].wait()
        firsts.append(pltpu.make_async_remote_copy(
            src_ref=head.at[i],
            dst_ref=out.at[0, r, pl.ds(0, HEAD), :, c],
            send_sem=send.at[15 * deep + i],
            recv_sem=recv.at[15 * deep + i],
            device_id=peers[bits][2],
        ))
        firsts[-1].start()
    for k in range(3):
        for bits in NEAR:
            pl.semaphore_signal(steps.at[k], inc=1, device_id=peers[bits][2])
        pl.semaphore_wait(steps.at[k], len(NEAR))

    queues, waiting, extra = [], [], []
    for side in range(2):
        queues.append([])
        for queue, flip in zip(QUEUES, FLIPS):
            queues[side].append([])
            for s in range(deep):
                for bits in queue:
                    bits ^= flip * side
                    low = HEAD if s == 0 and bits in FIRST else 0
                    high = tiles - HELD[0] if s == deep - 1 and bits // 4 % 2 == 0 else tiles
                    queues[side][-1].append(remote(bits, s, pl.ds(low, high - low), (bits - 1) * deep + s))
        waiting.append([list(queue) for queue in queues[side]])
    at = 15 * deep + len(FIRST)
    for bits in LATE:
        spans = cut(bits == 9, tiles - HELD[0], HELD[0] - HELD[1])
        extra.append((bits, [remote(bits, deep - 1, span, at + i) for i, span in enumerate(spans)]))
        at += len(spans)
    extra = dict(extra)

    def start(counts, side):
        for queue, count in zip(waiting[side], counts):
            for copy in queue[:count]:
                copy.start()
            del queue[:count]

    own_in = [pltpu.make_async_copy(x.at[s, c // 2, r, :, :, c % 2], own.at[s], osem.at[s])
              for s in range(deep)]
    own_out = [pltpu.make_async_copy(own.at[s], out.at[s, r, :, :, c], osem.at[s])
               for s in range(deep)]
    blocks = deep * 8

    def load(b):
        return pltpu.make_async_copy(x.at[b // 8, b // 4 % 2, b % 4], ring.at[b % 2], rsem.at[b % 2])

    def block(b, sq):
        load(b).wait()

        def column(e, sq):
            v = ring[b % 2, :, e]
            acc[e] += jnp.sum(v, axis=0)
            return sq + jnp.sum(v * v, axis=(0, 1))

        sq = lax.fori_loop(0, wide, column, sq)

        @pl.when(b + 2 < blocks)
        def _():
            load(b + 2).start()

        return sq

    by_core(core, functools.partial(start, STARTS[0]))
    load(0).start()
    load(1).start()
    for copy in own_in:
        copy.start()
    acc[...] = jnp.zeros_like(acc)
    sq = lax.fori_loop(0, blocks, block, jnp.zeros((SUB, SB), jnp.float32))
    part[...] = jnp.zeros_like(part)
    for k in range(2):
        for e in range(wide):
            part[k, e:e + 1, :] = jnp.sum(acc[e, k], axis=0, keepdims=True)
        part[k, wide:wide + 1, :] = jnp.sum(sq, axis=0, keepdims=True)
    for i in range(deep):
        own_in[i].wait()
        own_out[i].start()
    small = []
    for bits, (tr, tc, device) in peers.items():
        small.append(pltpu.make_async_remote_copy(
            src_ref=part.at[tc % 2], dst_ref=slots.at[me],
            send_sem=psend.at[bits], recv_sem=precv.at[bits], device_id=device,
        ))
        small[-1].start()
    slots[me] = part[c % 2]
    by_core(core, functools.partial(start, STARTS[1]))

    for copy in small:
        copy.wait()
    total = slots[0, wide:wide + 1, :]
    for i in range(1, 16):
        total += slots[i, wide:wide + 1, :]
    gsq[...] = jnp.broadcast_to(total, gsq.shape)
    for q in range(4):
        s = slots[q, :wide, :]
        for p in range(1, 4):
            s += slots[p * 4 + q, :wide, :]
        cols[pl.ds(q, wide, stride=4), :] = s * scale
    for copy in own_out:
        copy.wait()

    def finish(side):
        start([len(queue) for queue in waiting[side]], side)
        copies = firsts + [copy for queue in queues[side] for copy in queue]
        waited = []
        if side == 1:
            waited = chained(extra, queues[side][0][-1])
            copies += [copy for pieces in extra.values() for copy in pieces]
        settle_all(copies, waited)

    by_core(core, finish)


def settle(held, cols, gsq, out, cols_out, token, sem, tail):
    copies = [pltpu.make_async_copy(held.at[i // 4, i % 4], out.at[i // 4, i % 4], sem.at[i])
              for i in range(held.shape[0] * 4)]
    copies.append(pltpu.make_async_copy(cols, cols_out, tail))
    for copy in copies:
        copy.start()
    token[...] = gsq[...]
    for copy in copies:
        copy.wait()


def rest(groups, count, x, gsq, land, fro, gslots, send, recv, gsend, grecv):
    deep, _, _, tiles = x.shape[:4]
    r, c, group, peers, others = places(groups)
    core = c % 2

    barrier = pltpu.get_barrier_semaphore()
    for bits in LATE:
        pl.semaphore_signal(barrier, inc=1, device_id=peers[bits][2])
    for _, device in others:
        pl.semaphore_signal(barrier, inc=1, device_id=device)
    pl.semaphore_wait(barrier, len(LATE) + len(others))

    tail = []
    for i, device in others:
        tail.append(pltpu.make_async_remote_copy(
            src_ref=gsq, dst_ref=gslots.at[group],
            send_sem=gsend.at[i], recv_sem=grecv.at[i], device_id=device,
        ))
        tail[-1].start()
    gslots[group] = gsq[...]

    def exchange(side):
        pieces, at = {}, 0
        for bits in LATE:
            tr, tc, device = peers[bits]
            pieces[bits] = []
            for i, span in enumerate(cut(bits in (10, 11), 0, HELD[side])):
                pieces[bits].append(pltpu.make_async_remote_copy(
                    src_ref=x.at[deep - 1, tc // 2, tr, pl.ds(tiles - HELD[side] + span.start, span.size), :, tc % 2],
                    dst_ref=land.at[r, c // 2, span],
                    send_sem=send.at[at],
                    recv_sem=recv.at[at],
                    device_id=device,
                ))
                at += 1
        waited = paired(pieces)
        for copy in tail:
            copy.wait()
        total = gslots[0]
        for i in range(1, groups[0] * groups[1]):
            total += gslots[i]
        fro[...] = jnp.sqrt(jnp.broadcast_to(jnp.sum(total[0:1, :]) / count, fro.shape))
        settle_all([copy for copies in pieces.values() for copy in copies], waited)

    by_core(core, exchange)


def finish(land, fro, before, out, fro_out, scalar, sem, tail):
    del before
    deep, _, tiles = out.shape[:3]
    r, c, _, peers, _ = places((1, 1))

    def copies(side):
        moves = []
        for i, bits in enumerate(LATE):
            tr, tc, _ = peers[bits]
            moves.append(pltpu.make_async_copy(
                land.at[tr, tc // 2, pl.ds(0, HELD[side])],
                out.at[deep - 1, tr, pl.ds(tiles - HELD[side], HELD[side]), :, tc],
                sem.at[i],
            ))
        return moves

    def begin(side):
        for copy in copies(side):
            copy.start()

    def end(side):
        for copy in copies(side):
            copy.wait()

    by_core(c % 2, begin)
    scalar[0, 0] = jnp.max(fro[...])
    last = pltpu.make_async_copy(scalar, fro_out, tail)
    last.start()
    by_core(c % 2, end)
    last.wait()


def per_device(source_blocks):
    local_rows, local_cols = source_blocks.shape
    row_count, col_count = lax.axis_size("row"), lax.axis_size("col")
    groups = (row_count // 4, col_count // 4)
    total_rows = local_rows * row_count
    count = total_rows * local_cols * col_count
    deep, wide, tiles = local_rows // (8 * SB), local_cols // (2 * SB), SB // SUB
    x = source_blocks.reshape(local_rows // SUB, SUB, local_cols // SB, SB).transpose(0, 2, 1, 3)
    x = x.reshape(deep, 2, 4, tiles, wide, 2, SUB, SB)
    x = pltpu.with_memory_space_constraint(x, pltpu.HBM)
    f32 = jnp.float32
    rows = -(-(wide + 1) // SUB) * SUB
    n = groups[0] * groups[1]
    dma = pltpu.SemaphoreType.DMA
    anywhere = pl.BlockSpec(memory_space=pl.ANY)
    hbm = pl.BlockSpec(memory_space=pltpu.HBM)
    vmem = pl.BlockSpec(memory_space=pltpu.VMEM)
    small = jax.ShapeDtypeStruct((SUB, SB), f32)
    held, cols, gsq = pl.pallas_call(
        functools.partial(redistribute, groups, 1.0 / math.sqrt(total_rows)),
        out_shape=(
            pltpu.VMEM((deep, 4, tiles, wide, 4, SUB, SB), f32),
            jax.ShapeDtypeStruct((wide * 4, SB), f32),
            small,
        ),
        in_specs=[hbm],
        out_specs=(anywhere, vmem, vmem),
        scratch_shapes=[
            pltpu.VMEM((deep, tiles, wide, SUB, SB), f32),
            pltpu.VMEM((2, tiles, wide, 2, SUB, SB), f32),
            pltpu.VMEM((wide, 2, SUB, SB), f32),
            pltpu.VMEM((2, rows, SB), f32),
            pltpu.VMEM((16, rows, SB), f32),
            pltpu.VMEM((len(FIRST), HEAD, wide, SUB, SB), f32),
            dma((15 * deep + 12,)), dma((15 * deep + 12,)), dma((16,)), dma((16,)),
            pltpu.SemaphoreType.REGULAR((3,)), dma((deep,)), dma((2,)), dma((len(FIRST),)),
        ],
        compiler_params=pltpu.CompilerParams(
            collective_id=0, has_side_effects=True, vmem_limit_bytes=8 * 2**20
        ),
        name="redistribute",
    )(x)
    out, cols, token = pl.pallas_call(
        settle,
        out_shape=(pltpu.HBM(held.shape, f32), pltpu.HBM(cols.shape, f32), small),
        in_specs=[anywhere, vmem, vmem],
        out_specs=(hbm, hbm, vmem),
        scratch_shapes=[dma((deep * 4,)), dma(())],
        compiler_params=pltpu.CompilerParams(vmem_limit_bytes=2**20),
        name="settle",
    )(held, cols, gsq)
    land, fro = pl.pallas_call(
        functools.partial(rest, groups, float(count)),
        out_shape=(pltpu.VMEM((4, 2, max(HELD), wide, SUB, SB), f32), small),
        in_specs=[hbm, vmem],
        out_specs=(anywhere, vmem),
        scratch_shapes=[pltpu.VMEM((n, SUB, SB), f32), dma((9,)), dma((9,)), dma((n,)), dma((n,))],
        compiler_params=pltpu.CompilerParams(
            collective_id=1, has_side_effects=True, vmem_limit_bytes=2**20
        ),
        name="rest",
    )(x, token)
    out, fro = pl.pallas_call(
        finish,
        out_shape=(pltpu.HBM(out.shape, f32), pltpu.HBM((1, 1), f32)),
        in_specs=[anywhere, vmem, hbm],
        out_specs=(hbm, hbm),
        scratch_shapes=[pltpu.SMEM((1, 1), f32), dma((len(LATE),)), dma(())],
        input_output_aliases={2: 0},
        compiler_params=pltpu.CompilerParams(vmem_limit_bytes=2**20),
        name="finish",
    )(land, fro, out)
    target = out.reshape(deep * 4 * tiles, wide * 4, SUB, SB).transpose(0, 2, 1, 3)
    target = target.reshape(deep * 4 * SB, wide * 4 * SB)
    return target, cols.reshape(wide * 4 * SB), fro[0, 0]


def solution(mesh):
    return jax.shard_map(
        per_device,
        mesh=mesh,
        in_specs=(P("row", "col"),),
        out_specs=(P("row", "col"), P("col"), P()),
        check_vma=False,
    )
```

```python
import functools
import math

import jax
import jax.numpy as jnp
from jax import lax
from jax.experimental import pallas as pl
from jax.experimental.pallas import tpu as pltpu
from jax.sharding import PartitionSpec as P

SB = 128
SUB = 8
QUEUES = ((15, 8, 11, 12, 9, 10, 13, 14), (7, 2, 3, 6), (5, 1), (4,))
FLIPS = (3, 1, 0, 0)
STARTS = ((3, 2, 1, 1), (3, 1, 1, 0))
NEAR = (8, 2, 1, 4)
FIRST = (8, 2, 1)
HEAD = 4
LATE = (8, 11, 10, 9, 3, 1, 2)
HELD = (9, 1)
LEAD = 4


def flipped(index, bits):
    low = (index % 2 + bits % 2) % 2
    high = (index // 2 + bits // 2) % 2
    return high * 2 + low


def places(groups):
    me_row, me_col = lax.axis_index("row"), lax.axis_index("col")
    r, g = me_row % 4, me_row // 4
    c, h = me_col % 4, me_col // 4
    peers = {}
    for bits in range(1, 16):
        tr, tc = flipped(r, bits % 4), flipped(c, bits // 4)
        peers[bits] = (tr, tc, {"row": g * 4 + tr, "col": h * 4 + tc})
    others = []
    for dg in range(groups[0]):
        for dh in range(groups[1]):
            if dg or dh:
                og, oh = (g + dg) % groups[0], (h + dh) % groups[1]
                others.append((dg * groups[1] + dh, {"row": og * 4 + r, "col": oh * 4 + c}))
    return r, c, g * groups[1] + h, peers, others


def by_core(core, run):
    for side in range(2):
        pl.when(core == side)(functools.partial(run, side))


def chained(pieces, before):
    for bits in (8, 9, 10, 11):
        for copy in pieces[bits]:
            copy.start()
    before.wait_send()
    for bits in (3, 2):
        for copy in pieces[bits]:
            copy.start()
    pieces[9][0].wait_send()
    for copy in pieces[1]:
        copy.start()
    return [before, pieces[9][0]]


def paired(pieces):
    for bits in (8, 11, 10, 9, 3):
        for copy in pieces[bits]:
            copy.start()
    waited = []
    for gate, follower in ((11, 1), (10, 2)):
        pieces[gate][0].wait_send()
        waited.append(pieces[gate][0])
        for copy in pieces[follower]:
            copy.start()
    return waited


def settle_all(copies, waited):
    for copy in copies:
        if not any(copy is other for other in waited):
            copy.wait_send()
        copy.wait_recv()


def cut(split, start, many):
    if split and many > 1:
        lead = min(LEAD, many - 1)
        return [pl.ds(start, many - lead), pl.ds(start + many - lead, lead)]
    return [pl.ds(start, many)]


def redistribute(groups, scale, x, out, cols, gsq, own, ring, acc, part, slots, head,
                 send, recv, psend, precv, steps, osem, rsem, hsem):
    deep, _, _, tiles, wide = x.shape[:5]
    r, c, _, peers, _ = places(groups)
    me = r * 4 + c
    core = c % 2

    heads = []
    for i, bits in enumerate(FIRST):
        tr, tc, _ = peers[bits]
        heads.append(pltpu.make_async_copy(
            x.at[0, tc // 2, tr, pl.ds(0, HEAD), :, tc % 2], head.at[i], hsem.at[i]))
        heads[-1].start()

    def remote(bits, s, span, at):
        tr, tc, device = peers[bits]
        return pltpu.make_async_remote_copy(
            src_ref=x.at[s, tc // 2, tr, span, :, tc % 2],
            dst_ref=out.at[s, r, span, :, c],
            send_sem=send.at[at],
            recv_sem=recv.at[at],
            device_id=device,
        )

    barrier = pltpu.get_barrier_semaphore()
    for bits in NEAR:
        pl.semaphore_signal(barrier, inc=1, device_id=peers[bits][2])
    pl.semaphore_wait(barrier, len(NEAR))
    firsts = []
    for i, bits in enumerate(FIRST):
        heads[i].wait()
        firsts.append(pltpu.make_async_remote_copy(
            src_ref=head.at[i],
            dst_ref=out.at[0, r, pl.ds(0, HEAD), :, c],
            send_sem=send.at[15 * deep + i],
            recv_sem=recv.at[15 * deep + i],
            device_id=peers[bits][2],
        ))
        firsts[-1].start()
    for k in range(3):
        for bits in NEAR:
            pl.semaphore_signal(steps.at[k], inc=1, device_id=peers[bits][2])
        pl.semaphore_wait(steps.at[k], len(NEAR))

    queues, waiting, extra = [], [], []
    for side in range(2):
        queues.append([])
        for queue, flip in zip(QUEUES, FLIPS):
            queues[side].append([])
            for s in range(deep):
                for bits in queue:
                    bits ^= flip * side
                    low = HEAD if s == 0 and bits in FIRST else 0
                    high = tiles - HELD[0] if s == deep - 1 and bits // 4 % 2 == 0 else tiles
                    queues[side][-1].append(remote(bits, s, pl.ds(low, high - low), (bits - 1) * deep + s))
        waiting.append([list(queue) for queue in queues[side]])
    at = 15 * deep + len(FIRST)
    for bits in LATE:
        spans = cut(bits == 9, tiles - HELD[0], HELD[0] - HELD[1])
        extra.append((bits, [remote(bits, deep - 1, span, at + i) for i, span in enumerate(spans)]))
        at += len(spans)
    extra = dict(extra)

    def start(counts, side):
        for queue, count in zip(waiting[side], counts):
            for copy in queue[:count]:
                copy.start()
            del queue[:count]

    own_in = [pltpu.make_async_copy(x.at[s, c // 2, r, :, :, c % 2], own.at[s], osem.at[s])
              for s in range(deep)]
    own_out = [pltpu.make_async_copy(own.at[s], out.at[s, r, :, :, c], osem.at[s])
               for s in range(deep)]
    blocks = deep * 8

    def load(b):
        return pltpu.make_async_copy(x.at[b // 8, b // 4 % 2, b % 4], ring.at[b % 2], rsem.at[b % 2])

    def block(b, sq):
        load(b).wait()

        def column(e, sq):
            v = ring[b % 2, :, e]
            acc[e] += jnp.sum(v, axis=0)
            return sq + jnp.sum(v * v, axis=(0, 1))

        sq = lax.fori_loop(0, wide, column, sq)

        @pl.when(b + 2 < blocks)
        def _():
            load(b + 2).start()

        return sq

    by_core(core, functools.partial(start, STARTS[0]))
    load(0).start()
    load(1).start()
    for copy in own_in:
        copy.start()
    acc[...] = jnp.zeros_like(acc)
    sq = lax.fori_loop(0, blocks, block, jnp.zeros((SUB, SB), jnp.float32))
    part[...] = jnp.zeros_like(part)
    for k in range(2):
        for e in range(wide):
            part[k, e:e + 1, :] = jnp.sum(acc[e, k], axis=0, keepdims=True)
        part[k, wide:wide + 1, :] = jnp.sum(sq, axis=0, keepdims=True)
    for i in range(deep):
        own_in[i].wait()
        own_out[i].start()
    small = []
    for bits, (tr, tc, device) in peers.items():
        small.append(pltpu.make_async_remote_copy(
            src_ref=part.at[tc % 2], dst_ref=slots.at[me],
            send_sem=psend, recv_sem=precv, device_id=device,
        ))
        small[-1].start()
    slots[me] = part[c % 2]
    by_core(core, functools.partial(start, STARTS[1]))

    pltpu.make_async_remote_copy(
        src_ref=slots.at[pl.ds(0, len(small))], dst_ref=slots.at[pl.ds(0, len(small))],
        send_sem=psend, recv_sem=precv, device_id=peers[1][2],
    ).wait()
    total = slots[0, wide:wide + 1, :]
    for i in range(1, 16):
        total += slots[i, wide:wide + 1, :]
    gsq[...] = jnp.broadcast_to(total, gsq.shape)
    for q in range(4):
        s = slots[q, :wide, :]
        for p in range(1, 4):
            s += slots[p * 4 + q, :wide, :]
        cols[pl.ds(q, wide, stride=4), :] = s * scale
    for copy in own_out:
        copy.wait()

    def finish(side):
        start([len(queue) for queue in waiting[side]], side)
        copies = firsts + [copy for queue in queues[side] for copy in queue]
        waited = []
        if side == 1:
            waited = chained(extra, queues[side][0][-1])
            copies += [copy for pieces in extra.values() for copy in pieces]
        settle_all(copies, waited)

    by_core(core, finish)


def settle(held, cols, gsq, out, cols_out, token, sem, tail):
    copies = [pltpu.make_async_copy(held.at[i // 4, i % 4], out.at[i // 4, i % 4], sem.at[i])
              for i in range(held.shape[0] * 4)]
    copies.append(pltpu.make_async_copy(cols, cols_out, tail))
    for copy in copies:
        copy.start()
    token[...] = gsq[...]
    for copy in copies:
        copy.wait()


def rest(groups, count, x, gsq, land, fro, gslots, send, recv, gsend, grecv):
    deep, _, _, tiles = x.shape[:4]
    r, c, group, peers, others = places(groups)
    core = c % 2

    barrier = pltpu.get_barrier_semaphore()
    for bits in LATE:
        pl.semaphore_signal(barrier, inc=1, device_id=peers[bits][2])
    for _, device in others:
        pl.semaphore_signal(barrier, inc=1, device_id=device)
    pl.semaphore_wait(barrier, len(LATE) + len(others))

    tail = []
    for i, device in others:
        tail.append(pltpu.make_async_remote_copy(
            src_ref=gsq, dst_ref=gslots.at[group],
            send_sem=gsend.at[i], recv_sem=grecv.at[i], device_id=device,
        ))
        tail[-1].start()
    gslots[group] = gsq[...]

    def exchange(side):
        pieces, at = {}, 0
        for bits in LATE:
            tr, tc, device = peers[bits]
            pieces[bits] = []
            for i, span in enumerate(cut(bits in (10, 11), 0, HELD[side])):
                pieces[bits].append(pltpu.make_async_remote_copy(
                    src_ref=x.at[deep - 1, tc // 2, tr, pl.ds(tiles - HELD[side] + span.start, span.size), :, tc % 2],
                    dst_ref=land.at[r, c // 2, span],
                    send_sem=send.at[at],
                    recv_sem=recv.at[at],
                    device_id=device,
                ))
                at += 1
        waited = paired(pieces)
        for copy in tail:
            copy.wait()
        total = gslots[0]
        for i in range(1, groups[0] * groups[1]):
            total += gslots[i]
        fro[...] = jnp.sqrt(jnp.broadcast_to(jnp.sum(total[0:1, :]) / count, fro.shape))
        settle_all([copy for copies in pieces.values() for copy in copies], waited)

    by_core(core, exchange)


def finish(land, fro, before, out, fro_out, scalar, sem, tail):
    del before
    deep, _, tiles = out.shape[:3]
    r, c, _, peers, _ = places((1, 1))

    def copies(side):
        moves = []
        for i, bits in enumerate(LATE):
            tr, tc, _ = peers[bits]
            moves.append(pltpu.make_async_copy(
                land.at[tr, tc // 2, pl.ds(0, HELD[side])],
                out.at[deep - 1, tr, pl.ds(tiles - HELD[side], HELD[side]), :, tc],
                sem.at[i],
            ))
        return moves

    def begin(side):
        for copy in copies(side):
            copy.start()

    def end(side):
        for copy in copies(side):
            copy.wait()

    by_core(c % 2, begin)
    scalar[0, 0] = jnp.max(fro[...])
    last = pltpu.make_async_copy(scalar, fro_out, tail)
    last.start()
    by_core(c % 2, end)
    last.wait()


def per_device(source_blocks):
    local_rows, local_cols = source_blocks.shape
    row_count, col_count = lax.axis_size("row"), lax.axis_size("col")
    groups = (row_count // 4, col_count // 4)
    total_rows = local_rows * row_count
    count = total_rows * local_cols * col_count
    deep, wide, tiles = local_rows // (8 * SB), local_cols // (2 * SB), SB // SUB
    x = source_blocks.reshape(local_rows // SUB, SUB, local_cols // SB, SB).transpose(0, 2, 1, 3)
    x = x.reshape(deep, 2, 4, tiles, wide, 2, SUB, SB)
    x = pltpu.with_memory_space_constraint(x, pltpu.HBM)
    f32 = jnp.float32
    rows = -(-(wide + 1) // SUB) * SUB
    n = groups[0] * groups[1]
    dma = pltpu.SemaphoreType.DMA
    anywhere = pl.BlockSpec(memory_space=pl.ANY)
    hbm = pl.BlockSpec(memory_space=pltpu.HBM)
    vmem = pl.BlockSpec(memory_space=pltpu.VMEM)
    small = jax.ShapeDtypeStruct((SUB, SB), f32)
    held, cols, gsq = pl.pallas_call(
        functools.partial(redistribute, groups, 1.0 / math.sqrt(total_rows)),
        out_shape=(
            pltpu.VMEM((deep, 4, tiles, wide, 4, SUB, SB), f32),
            jax.ShapeDtypeStruct((wide * 4, SB), f32),
            small,
        ),
        in_specs=[hbm],
        out_specs=(anywhere, vmem, vmem),
        scratch_shapes=[
            pltpu.VMEM((deep, tiles, wide, SUB, SB), f32),
            pltpu.VMEM((2, tiles, wide, 2, SUB, SB), f32),
            pltpu.VMEM((wide, 2, SUB, SB), f32),
            pltpu.VMEM((2, rows, SB), f32),
            pltpu.VMEM((16, rows, SB), f32),
            pltpu.VMEM((len(FIRST), HEAD, wide, SUB, SB), f32),
            dma((15 * deep + 11,)), dma((15 * deep + 11,)), dma(()), dma(()),
            pltpu.SemaphoreType.REGULAR((3,)), dma((deep,)), dma((2,)), dma((len(FIRST),)),
        ],
        compiler_params=pltpu.CompilerParams(
            collective_id=0, has_side_effects=True, vmem_limit_bytes=8 * 2**20
        ),
        name="redistribute",
    )(x)
    out, cols, token = pl.pallas_call(
        settle,
        out_shape=(pltpu.HBM(held.shape, f32), pltpu.HBM(cols.shape, f32), small),
        in_specs=[anywhere, vmem, vmem],
        out_specs=(hbm, hbm, vmem),
        scratch_shapes=[dma((deep * 4,)), dma(())],
        compiler_params=pltpu.CompilerParams(vmem_limit_bytes=2**20),
        name="settle",
    )(held, cols, gsq)
    land, fro = pl.pallas_call(
        functools.partial(rest, groups, float(count)),
        out_shape=(pltpu.VMEM((4, 2, max(HELD), wide, SUB, SB), f32), small),
        in_specs=[hbm, vmem],
        out_specs=(anywhere, vmem),
        scratch_shapes=[pltpu.VMEM((n, SUB, SB), f32), dma((9,)), dma((9,)), dma((n,)), dma((n,))],
        compiler_params=pltpu.CompilerParams(
            collective_id=1, has_side_effects=True, vmem_limit_bytes=2**20
        ),
        name="rest",
    )(x, token)
    out, fro = pl.pallas_call(
        finish,
        out_shape=(pltpu.HBM(out.shape, f32), pltpu.HBM((1, 1), f32)),
        in_specs=[anywhere, vmem, hbm],
        out_specs=(hbm, hbm),
        scratch_shapes=[pltpu.SMEM((1, 1), f32), dma((len(LATE),)), dma(())],
        input_output_aliases={2: 0},
        compiler_params=pltpu.CompilerParams(vmem_limit_bytes=2**20),
        name="finish",
    )(land, fro, out)
    target = out.reshape(deep * 4 * tiles, wide * 4, SUB, SB).transpose(0, 2, 1, 3)
    target = target.reshape(deep * 4 * SB, wide * 4 * SB)
    return target, cols.reshape(wide * 4 * SB), fro[0, 0]


def solution(mesh):
    return jax.shard_map(
        per_device,
        mesh=mesh,
        in_specs=(P("row", "col"),),
        out_specs=(P("row", "col"), P("col"), P()),
        check_vma=False,
    )
```
